32 devices in a mesh: pair: 4 (over y, x), grow: 4 (over z), gcol: 2 (over core).
Axes of the slice: x: 2, y: 2, z: 4, core: 2. Of those that a mesh axis runs over, the one named last changes fastest.
Arguments:
- valence: bfloat16 [16, 96, 9216], P(None, 'grow'), may hold values from -6 to 6
- conduction: bfloat16 [16, 96, 9216], P(('pair', 'gcol'), 'grow'), may hold values from -6 to 6
- val_energy: float32 [16], replicated, may hold values from -10 to -1
- cond_energy: float32 [16], replicated, may hold values from 1 to 20
- val_occupation: int32 [16], replicated, may hold values from 1 to 16
- gvectors: int32 [3, 3840], replicated, may hold values from -12 to 12, as said below
Outputs:
- chi_zero: float32 [7680, 7680], P(('pair', 'gcol'), 'grow')
The draws below stay inside these ranges and needn't reach their ends.
Inputs may be any that keep to these rules, and one draw needn't show every extreme that they name: gvectors holds 3840 distinct wave vectors; the first component lies in 1 .. 12, the other two in -12 .. 12.
All inputs are finite; a program needn't handle non-finite values.
Results may differ from the reference program's by a relative error of at most 0.02.
Values may be sent and summed in bfloat16 or wider, within the bound.
A program may use at most 128 MiB of HBM per device.

```python
import math
import jax
import jax.numpy as jnp
from jax import lax

N = 96
RAD = 12
KG = 3840
NV = 16
NCOND = 16
NPAIRS = 256
N_GROW = 4


def draw_gvectors(key, part):
    extent = 2 * RAD + 1
    total_count = RAD * extent * extent
    chosen = jax.random.permutation(jax.random.fold_in(key, 11), total_count)[:KG]
    component_a = chosen // (extent * extent) + 1
    component_b = chosen // extent % extent - RAD
    component_c = chosen % extent - RAD
    return jnp.stack([component_a, component_b, component_c]).astype(jnp.int32)


def touch_ends(array, key, low, top_value):
    place = [jax.random.randint(jax.random.fold_in(key, axis), (), 0, length) for axis, length in enumerate(array.shape)]
    main_axis = array.shape.index(max(array.shape))
    neighbour = place[:main_axis] + [(place[main_axis] + 1) % array.shape[main_axis]] + place[main_axis + 1:]
    return array.at[tuple(place)].set(low).at[tuple(neighbour)].set(top_value)


def steps_of(rng, shape, pieces, low, top_value):
    def one(axis_at, parts):
        steps = jax.random.uniform(jax.random.fold_in(jax.random.fold_in(rng, 6), axis_at), (parts,), jnp.float32, low / len(pieces), top_value / len(pieces))
        return jnp.repeat(jnp.exp(steps), shape[axis_at] // parts).reshape((-1,) + (1,) * (len(shape) - axis_at - 1))

    level = one(*pieces[0])
    for cut in pieces[1:]:
        level = level * one(*cut)
    return level


def scatter_about(key, shape, deviation, reach, cuts=(), kind=jnp.bfloat16):
    gain = steps_of(key, shape, cuts, -0.22, 0.18) if cuts else 1.0
    array = jax.random.normal(key, shape, jnp.float32) * deviation * gain
    return jnp.minimum(jnp.maximum(array, -reach), reach).astype(kind)


def setup_inputs(seed: int = 0) -> dict:
    arg_keys = jax.random.split(jax.random.key(seed), 7)
    valence = scatter_about(arg_keys[0], (NV, N, N * N), 1.0, 6.0, ((1, 4),))
    conduction = scatter_about(arg_keys[1], (NCOND, N, N * N), 1.0, 6.0, ((0, 8), (1, 4)))
    val_energy = jnp.clip(jax.random.uniform(arg_keys[2], (NV,), jnp.float32, -10.0, -1.0), -10.0, -1.0)
    cond_energy = jnp.clip(jax.random.uniform(arg_keys[3], (NCOND,), jnp.float32, 1.0, 20.0), 1.0, 20.0)
    val_occupation = touch_ends(jax.random.randint(arg_keys[4], (NV,), 1, 17), jax.random.fold_in(arg_keys[4], 1), 1, 16).astype(jnp.int32)
    gvectors = draw_gvectors(jax.random.fold_in(arg_keys[6], 71), 0)
    return dict(valence=valence, conduction=conduction, val_energy=val_energy, cond_energy=cond_energy, val_occupation=val_occupation, gvectors=gvectors)


def wave_tables(positions, frequencies):
    phases = jnp.mod(positions[:, None] * frequencies[None, :], N).astype(jnp.float32) * (2.0 * math.pi / N)
    return (jnp.cos(phases), jnp.sin(phases))

def build_tables(x_positions):
    all_freq = jnp.arange(-RAD, RAD + 1, dtype=jnp.int32)
    pos_freq = jnp.arange(1, RAD + 1, dtype=jnp.int32)
    positions = jnp.arange(N, dtype=jnp.int32)
    cosine, sine_part = wave_tables(positions, all_freq)
    z_table = jnp.concatenate([cosine, sine_part], 1).astype(jnp.bfloat16)
    y_table = jnp.stack([jnp.stack([cosine, sine_part], 1), jnp.stack([-sine_part, cosine], 1)], 1).astype(jnp.bfloat16)
    x_cos, x_sin = wave_tables(x_positions, pos_freq)
    x_table = jnp.stack([jnp.stack([x_cos, -x_sin], 1), jnp.stack([-x_sin, -x_cos], 1)], 1).astype(jnp.bfloat16)
    return (z_table, y_table, x_table)

def band_transform(one_band, valence, z_table, y_table, x_table, flat_index):
    extent = 2 * RAD + 1
    planes = N // N_GROW
    density = valence * one_band[None]
    section_one = jnp.dot(density.reshape(-1, N), z_table, preferred_element_type=jnp.float32).astype(jnp.bfloat16)
    section_one = section_one.reshape(NV * N, N, 2, extent)
    second = jnp.einsum('ayik,yioj->aojk', section_one.astype(jnp.float32), y_table.astype(jnp.float32)).astype(jnp.bfloat16)
    second = second.reshape(NV, N_GROW, planes, 2, extent * extent)
    block_table = x_table.reshape(N_GROW, planes, 2, 2, RAD)
    blocks = jnp.einsum('pbxoq,bxosm->pbsmq', second.astype(jnp.float32), block_table.astype(jnp.float32))
    rounded = lax.optimization_barrier(blocks.astype(jnp.bfloat16))
    section_three = lax.optimization_barrier(jnp.sum(rounded.astype(jnp.float32), axis=1))
    section_three = section_three.reshape(NV, 2, RAD * extent * extent)
    picked = jnp.take(section_three, flat_index, axis=2)
    return picked.reshape(NV, 2 * KG)

def reference(valence, conduction, val_energy, cond_energy, val_occupation, gvectors):
    extent = 2 * RAD + 1
    z_table, y_table, x_table = build_tables(jnp.arange(N, dtype=jnp.int32))
    flat_index = (((gvectors[0] - 1) * extent + gvectors[1] + RAD) * extent + gvectors[2] + RAD).astype(jnp.int32)
    weight = val_occupation.astype(jnp.float32)[None, :] / (4.0 * (cond_energy[:, None] - val_energy[None, :]))
    factor = jnp.sqrt(weight) * (1.0 / N ** 1.5)

    def per_band(inputs):
        one_band, band_factor = inputs
        picked = band_transform(one_band, valence, z_table, y_table, x_table, flat_index)
        return (picked * band_factor[:, None]).astype(jnp.bfloat16)
    weighted = lax.map(per_band, (conduction, factor))
    flattened = weighted.reshape(-1, 2 * KG)
    chi_block = lax.dot_general(flattened, flattened, (((0,), (0,)), ((), ())), preferred_element_type=jnp.float32)
    return chi_block * (-1.0 / math.sqrt(NPAIRS))
```

```python
import math

import functools

import jax
import jax.numpy as jnp
import numpy as np
from jax import lax
from jax.experimental import pallas as pl
from jax.experimental.pallas import tpu as pltpu
from jax.sharding import PartitionSpec as P

N = 96
RAD = 12
KG = 3840
NV = 16


def wave_tables(positions, frequencies):
    phases = jnp.mod(positions[:, None] * frequencies[None, :], N).astype(jnp.float32) * (
        2.0 * math.pi / N
    )
    return (jnp.cos(phases), jnp.sin(phases))


def build_tables(x_positions):
    all_freq = jnp.arange(-RAD, RAD + 1, dtype=jnp.int32)
    pos_freq = jnp.arange(1, RAD + 1, dtype=jnp.int32)
    positions = jnp.arange(N, dtype=jnp.int32)
    cosine, sine_part = wave_tables(positions, all_freq)
    z_table = jnp.concatenate([cosine, sine_part], 1).astype(jnp.bfloat16)
    y_table = jnp.stack(
        [jnp.stack([cosine, sine_part], 1), jnp.stack([-sine_part, cosine], 1)], 1
    ).astype(jnp.bfloat16)
    x_cos, x_sin = wave_tables(x_positions, pos_freq)
    x_table = jnp.stack([jnp.stack([x_cos, -x_sin], 1), jnp.stack([-x_sin, -x_cos], 1)], 1).astype(
        jnp.bfloat16
    )
    return (z_table, y_table, x_table)


def pair_product(left_rows, right_rows):
    return lax.dot_general(
        left_rows, right_rows, (((0,), (0,)), ((), ())), preferred_element_type=jnp.float32
    )


def body(valence, conduction, val_energy, cond_energy, val_occupation, gvectors):
    pair_count = lax.axis_size("pair")
    gcol_count = lax.axis_size("gcol")
    planes = valence.shape[1]
    cond_bands = conduction.shape[0]
    extent = 2 * RAD + 1
    local_pairs = cond_bands * NV
    x_positions = lax.axis_index("grow") * planes + jnp.arange(planes, dtype=jnp.int32)
    z_table, y_table, x_table = build_tables(x_positions)
    flat_index = ((gvectors[0] - 1) * extent + gvectors[1] + RAD) * extent + gvectors[2] + RAD
    density = conduction[:, None] * valence[None]
    section_one = jnp.dot(
        density.reshape(-1, N), z_table, preferred_element_type=jnp.float32
    ).astype(jnp.bfloat16)
    section_one = section_one.reshape(local_pairs * planes, N, 2, extent)
    second = jnp.einsum(
        "ayik,yioj->aojk", section_one, y_table, preferred_element_type=jnp.float32
    ).astype(jnp.bfloat16)
    second = second.reshape(local_pairs, planes, 2, extent * extent)
    section_three = jnp.einsum(
        "pxoq,xosm->psmq", second, x_table, preferred_element_type=jnp.float32
    )
    section_three = section_three.reshape(local_pairs, 2, RAD * extent * extent)
    picked = jnp.take(section_three, flat_index, axis=2).reshape(local_pairs, 2 * KG)
    summed = lax.psum_scatter(
        picked.astype(jnp.bfloat16), "grow", scatter_dimension=1, tiled=True
    ).astype(jnp.float32)
    first_band = (lax.axis_index("pair") * gcol_count + lax.axis_index("gcol")) * cond_bands
    own_energy = lax.dynamic_slice_in_dim(cond_energy, first_band, cond_bands, 0)
    weight = val_occupation.astype(jnp.float32)[None, :] / (
        4.0 * (own_energy[:, None] - val_energy[None, :])
    )
    factor = (jnp.sqrt(weight) * (1.0 / N**1.5)).reshape(local_pairs, 1)
    weighted = (summed * factor).astype(jnp.bfloat16)
    prefactor = -1.0 / math.sqrt(pair_count * gcol_count * local_pairs)
    full_rows = lax.all_gather(weighted, "grow", axis=1, tiled=True)
    row_part = lax.all_to_all(full_rows, "pair", split_axis=1, concat_axis=0, tiled=True)
    partial_value = pair_product(row_part, lax.all_gather(weighted, "pair", axis=0, tiled=True))
    return lax.psum_scatter(
        (partial_value * prefactor).astype(jnp.bfloat16), "gcol", scatter_dimension=0, tiled=True
    ).astype(jnp.float32)


EXT = 2 * RAD + 1
QUARTER = N * N // 4
STEP = 8 * N
CLASSES = ((0, 4, 8, 12), (2, 6, 10), (1, 3, 5, 7, 9, 11))
WIDTHS = (128, 128, 256)
ROWS = (104, 80, 152)
STARTS = (0, 104, 184)
NR = 336


def half_plane_tables():
    total = 2 * sum(WIDTHS)
    left = np.zeros((2, N // 4, total), np.float32)
    right = np.zeros((2, N, total), np.float32)
    sign = np.zeros((1, WIDTHS[2]), np.float32)
    y = np.arange(N // 4)[:, None]
    z = np.arange(N)[:, None]
    k = np.arange(-RAD, RAD + 1)
    base = 0
    for freqs, width in zip(CLASSES, WIDTHS):
        jj = np.repeat(np.array(freqs), EXT)[None]
        kk = np.tile(k, len(freqs))[None]
        count = jj.shape[1]
        ay = 2 * np.pi * ((jj * y) % N) / N
        az = 2 * np.pi * ((kk * z) % N) / N
        for part in range(2):
            cols = slice(base + part * width, base + part * width + count)
            left[0, :, cols] = np.sin(ay) if part else np.cos(ay)
            left[1, :, cols] = np.cos(ay) if part else -np.sin(ay)
            right[0, :, cols] = np.cos(az)
            right[1, :, cols] = np.sin(az)
        base += 2 * width
    jj = np.repeat(np.array(CLASSES[2]), EXT)
    sign[0, : jj.size] = np.where(jj % 4 == 1, 1.0, -1.0)
    return left, right, sign


def plane_table(pairs):
    x = np.arange(N)[:, None]
    a = np.arange(1, RAD + 1)[None]
    ang = 2 * np.pi * ((a * x) % N) / N
    c, s = np.cos(ang), np.sin(ang)
    tab = np.stack([np.stack([c, -s, c, -s], -1), np.stack([-s, -c, s, c], -1)])
    return np.repeat(tab.reshape(2, N, RAD * 4), pairs, axis=2).astype(np.float32)


def transform_kernel(
    idx, grow, v0, v1, v2, v3, c0, c1, c2, c3, left, right, sign, xtab, factor, out,
    ee, eo, oo, tab, acc_ee, acc_eo, acc_o, xmat, sec, got,
):
    step = pl.program_id(0)
    nv, planes, _ = v0.shape
    bands = c0.shape[0]
    pairs = nv * bands
    rows = pairs * planes
    lanes = 4 * pairs
    f32 = jnp.float32

    @pl.when(step == 0)
    def _():
        acc_ee[...] = jnp.zeros_like(acc_ee)
        acc_eo[...] = jnp.zeros_like(acc_eo)
        acc_o[...] = jnp.zeros_like(acc_o)

    for y in range(STEP // N):
        yy = step * (STEP // N) + y
        l1 = left[0, pl.ds(yy, 1), :]
        l2 = left[1, pl.ds(yy, 1), :]
        tab[y * N : (y + 1) * N, :] = (l1 * right[0] + l2 * right[1]).astype(jnp.bfloat16)

    def products(v, carry):
        vals = [ref[pl.ds(2 * v, 2)].astype(f32) for ref in (v0, v1, v2, v3)]
        for c in range(bands):
            d0, d1, d2, d3 = [
                (val * ref[c].astype(f32)[None]).reshape(2 * planes, STEP)
                for val, ref in zip(vals, (c0, c1, c2, c3))
            ]
            e0, e1 = d0 + d2, d1 + d3
            at = pl.multiple_of(c * nv * planes + v * 2 * planes, 16)
            where = pl.ds(at, 2 * planes)
            ee[where, :] = (e0 + e1).astype(jnp.bfloat16)
            eo[where, :] = (e0 - e1).astype(jnp.bfloat16)
            oo[where, :] = (d0 - d2).astype(jnp.bfloat16)
            oo[pl.ds(pl.multiple_of(rows + at, 16), 2 * planes), :] = (d1 - d3).astype(jnp.bfloat16)
        return carry

    lax.fori_loop(0, nv // 2, products, 0)

    def multiply(i, carry):
        block = rows // 2
        part = pl.ds(pl.multiple_of(i * block, 16), block)
        acc_ee[part, :] += jnp.dot(ee[part, :], tab[:, 0:256], preferred_element_type=f32)
        acc_eo[part, :] += jnp.dot(eo[part, :], tab[:, 256:512], preferred_element_type=f32)
        for h in range(2):
            at = pl.ds(pl.multiple_of(h * rows + i * block, 16), block)
            acc_o[at, :] += jnp.dot(oo[at, :], tab[:, 512:1024], preferred_element_type=f32)
        return carry

    lax.fori_loop(0, 2, multiply, 0)

    @pl.when(step == pl.num_programs(0) - 1)
    def _():
        own = lax.broadcasted_iota(jnp.int32, (1, RAD * lanes), 1) % pairs

        def place(p, carry):
            for h in range(2):
                two = []
                for u in range(2):
                    two.append(jnp.where(own == 2 * p + u, xtab[h], 0.0))
                at = pl.multiple_of(h * rows + p * 2 * planes, 16)
                xmat[pl.ds(at, 2 * planes), :] = jnp.concatenate(two, 0).astype(jnp.bfloat16)
            return carry

        lax.fori_loop(0, pairs // 2, place, 0)
        w = WIDTHS[2]
        top, low = acc_o[0:rows, :], acc_o[rows : 2 * rows, :]
        odd_p = top[:, 0:w] - sign[...] * low[:, w:]
        odd_q = top[:, w:] + sign[...] * low[:, 0:w]
        groups = (
            (acc_ee[:, 0:128], acc_ee[:, 128:256]),
            (acc_eo[:, 0:128], acc_eo[:, 128:256]),
            (odd_p, odd_q),
        )
        for (p_part, q_part), count, start in zip(groups, ROWS, STARTS):
            p_rows = p_part.T[0:count].astype(jnp.bfloat16)
            q_rows = q_part.T[0:count].astype(jnp.bfloat16)
            summed = jnp.dot(p_rows, xmat[0:rows, :], preferred_element_type=f32)
            summed += jnp.dot(q_rows, xmat[rows : 2 * rows, :], preferred_element_type=f32)
            for a in range(RAD):
                piece = summed[:, a * lanes : (a + 1) * lanes] * factor[...]
                sec[a * NR + start : a * NR + start + count, :] = piece
                at = (RAD + a) * NR + start
                sec[at : at + count, :] = pltpu.roll(piece, lanes // 2, 1)

        def pick(i, carry):
            for u in range(16):
                got[pl.ds(i * 16 + u, 1), :] = sec[pl.ds(idx[i * 16 + u], 1), :]
            return carry

        lax.fori_loop(0, KG // 16, pick, 0)
        for i in range(KG // 384):
            turned = got[i * 384 : (i + 1) * 384, :].T.astype(jnp.bfloat16)
            out[:, i * 384 : (i + 1) * 384] = turned[0:pairs]
            out[:, KG + i * 384 : KG + (i + 1) * 384] = turned[pairs : 2 * pairs]


def pair_transform(valence, conduction, factor, gvectors):
    nv, planes, _ = valence.shape
    bands = conduction.shape[0]
    pairs = nv * bands
    rows = pairs * planes
    lanes = 4 * pairs
    steps = QUARTER // STEP
    a, b, d = gvectors[0], gvectors[1], gvectors[2]
    flip = b < 0
    j = jnp.abs(b)
    k = jnp.where(flip, -d, d) + RAD
    row = jnp.where(
        j % 2 == 1,
        STARTS[2] + (j // 2) * EXT,
        jnp.where(j % 4 == 2, STARTS[1], STARTS[0]) + (j // 4) * EXT,
    )
    index = (jnp.where(flip, RAD, 0) + a - 1) * NR + row + k
    grow = lax.axis_index("grow").astype(jnp.int32).reshape(1)
    left, right, sign = half_plane_tables()
    whole = lambda shape: pl.BlockSpec(shape, lambda i, idx, g: (0,) * len(shape))
    piece = lambda n, q: pl.BlockSpec(
        (n, planes, STEP), lambda i, idx, g, q=q: (0, 0, q * steps + i)
    )
    call = pl.pallas_call(
        transform_kernel,
        out_shape=jax.ShapeDtypeStruct((pairs, 2 * KG), jnp.bfloat16),
        grid_spec=pltpu.PrefetchScalarGridSpec(
            num_scalar_prefetch=2,
            grid=(steps,),
            in_specs=[piece(nv, q) for q in range(4)]
            + [piece(bands, q) for q in range(4)]
            + [
                whole(left.shape),
                whole(right.shape),
                whole(sign.shape),
                pl.BlockSpec((2, planes, RAD * lanes), lambda i, idx, g: (0, g[0], 0)),
                whole((1, lanes)),
            ],
            out_specs=whole((pairs, 2 * KG)),
            scratch_shapes=[
                pltpu.VMEM((rows, STEP), jnp.bfloat16),
                pltpu.VMEM((rows, STEP), jnp.bfloat16),
                pltpu.VMEM((2 * rows, STEP), jnp.bfloat16),
                pltpu.VMEM((STEP, 2 * sum(WIDTHS)), jnp.bfloat16),
                pltpu.VMEM((rows, 2 * WIDTHS[0]), jnp.float32),
                pltpu.VMEM((rows, 2 * WIDTHS[1]), jnp.float32),
                pltpu.VMEM((2 * rows, 2 * WIDTHS[2]), jnp.float32),
                pltpu.VMEM((2 * rows, RAD * lanes), jnp.bfloat16),
                pltpu.VMEM((2 * RAD * NR, lanes), jnp.float32),
                pltpu.VMEM((KG, lanes), jnp.float32),
            ],
        ),
        compiler_params=pltpu.CompilerParams(vmem_limit_bytes=60 * 1024 * 1024),
    )
    return call(
        index, grow, *([valence] * 4), *([conduction] * 4), left, right, sign,
        plane_table(pairs), jnp.tile(factor.reshape(1, pairs), (1, 4)),
    )


def exchange_kernel(
    part, cols, rows, inbox, blocks, sends, recvs,
):
    count, _, width = blocks.shape
    p, g, c = lax.axis_index("pair"), lax.axis_index("grow"), lax.axis_index("gcol")
    me = p * 2 + c
    f32 = jnp.float32
    turn = lambda at, k: lax.rem(at + k, count)
    barrier = pltpu.get_barrier_semaphore()
    for k in range(1, count):
        pl.semaphore_signal(barrier, inc=1, device_id=(p, turn(g, k), c))
        pl.semaphore_signal(barrier, inc=1, device_id=(turn(p, k), g, c))
    pl.semaphore_signal(barrier, inc=1, device_id=(p, g, 1 - c))
    pl.semaphore_wait(barrier, 2 * count - 1)

    def send(src, dst, sem, to):
        copy = pltpu.make_async_remote_copy(
            src_ref=src, dst_ref=dst, send_sem=sends.at[sem], recv_sem=recvs.at[sem],
            device_id=to, device_id_type=pl.DeviceIdType.MESH,
        )
        copy.start()
        return copy

    block = lambda at: pl.ds(pl.multiple_of(at * width, 128), width)
    first = [
        send(part.at[:, block(turn(g, k))], inbox.at[k - 1], k - 1, (p, turn(g, k), c))
        for k in range(1, count)
    ]
    total = part[:, block(g)].astype(f32)
    for k in range(1, count):
        first[k - 1].wait_recv()
        total += inbox[k - 1].astype(f32)
    mine = total.astype(jnp.bfloat16)
    blocks[g] = mine
    cols[me] = mine
    n = count - 1
    along = [
        send(blocks.at[g], blocks.at[g], n + k - 1, (p, turn(g, k), c)) for k in range(1, count)
    ]
    flat = [
        send(cols.at[me], cols.at[me], 2 * n + k - 1, (turn(p, k), g, c)) for k in range(1, count)
    ]
    over = [send(cols.at[me], cols.at[me], 4 * n, (p, g, 1 - c))]
    for copy in along:
        copy.wait_recv()
    across = [
        send(blocks.at[turn(p, k)], rows.at[me], 3 * n + k - 1, (turn(p, k), g, c))
        for k in range(1, count)
    ]
    rows[me] = blocks[p]
    over.append(send(rows.at[me], rows.at[me], 4 * n + 1, (p, g, 1 - c)))
    for k in range(1, count):
        slot = turn(p, count - k) * 2 + c
        flat[k - 1].wait_recv()
        over.append(send(cols.at[slot], cols.at[slot], 4 * n + 1 + k, (p, g, 1 - c)))
    for k in range(1, count):
        slot = turn(p, count - k) * 2 + c
        across[k - 1].wait_recv()
        over.append(send(rows.at[slot], rows.at[slot], 5 * n + 1 + k, (p, g, 1 - c)))
    for copy in over:
        copy.wait_recv()
    for copy in first + along + flat + across + over:
        copy.wait_send()


def exchange(part, count):
    pairs, total = part.shape
    width = total // count
    gathered = jax.ShapeDtypeStruct((2 * count, pairs, width), jnp.bfloat16)
    vmem = pl.BlockSpec(memory_space=pltpu.VMEM)
    sems = 6 * (count - 1) + 2
    return pl.pallas_call(
        exchange_kernel,
        out_shape=(gathered, gathered),
        in_specs=[vmem],
        out_specs=(vmem, vmem),
        scratch_shapes=[
            pltpu.VMEM((count - 1, pairs, width), jnp.bfloat16),
            pltpu.VMEM((count, pairs, width), jnp.bfloat16),
            pltpu.SemaphoreType.DMA((sems,)),
            pltpu.SemaphoreType.DMA((sems,)),
        ],
        compiler_params=pltpu.CompilerParams(collective_id=0, has_side_effects=True),
    )(part)


def fast_body(valence, conduction, val_energy, cond_energy, val_occupation, gvectors):
    pair_count = lax.axis_size("pair")
    gcol_count = lax.axis_size("gcol")
    cond_bands = conduction.shape[0]
    local_pairs = cond_bands * valence.shape[0]
    first_band = (lax.axis_index("pair") * gcol_count + lax.axis_index("gcol")) * cond_bands
    own_energy = lax.dynamic_slice_in_dim(cond_energy, first_band, cond_bands, 0)
    weight = val_occupation.astype(jnp.float32)[None, :] / (
        4.0 * (own_energy[:, None] - val_energy[None, :])
    )
    factor = (jnp.sqrt(weight) * (1.0 / N**1.5)).reshape(local_pairs)
    part = pair_transform(valence, conduction, factor, gvectors)
    prefactor = -1.0 / math.sqrt(pair_count * gcol_count * local_pairs)
    cols, rows = exchange(part, pair_count)
    all_pairs = pair_count * gcol_count * local_pairs
    cols = cols.reshape(all_pairs, -1)
    rows = rows.reshape(all_pairs, -1)
    height = rows.shape[1] // gcol_count
    rows = lax.dynamic_slice_in_dim(rows, lax.axis_index("gcol") * height, height, 1)
    return pair_product(rows, cols) * prefactor


def solution(mesh):
    sizes = dict(mesh.shape)
    fast = sizes["pair"] == sizes["grow"] and sizes["gcol"] == 2 and N // sizes["grow"] % 8 == 0
    return jax.shard_map(
        fast_body if fast else body,
        mesh=mesh,
        in_specs=(P(None, "grow", None), P(("pair", "gcol"), "grow", None), P(), P(), P(), P()),
        out_specs=P(("pair", "gcol"), "grow"),
        check_vma=False,
    )
```

```python
import math

import jax
import jax.numpy as jnp
import numpy as np
from jax import lax
from jax.experimental import pallas as pl
from jax.experimental.pallas import tpu as pltpu
from jax.sharding import PartitionSpec as P

N = 96
RAD = 12
KG = 3840
NV = 16


def wave_tables(positions, frequencies):
    phases = jnp.mod(positions[:, None] * frequencies[None, :], N).astype(jnp.float32) * (
        2.0 * math.pi / N
    )
    return (jnp.cos(phases), jnp.sin(phases))


def build_tables(x_positions):
    all_freq = jnp.arange(-RAD, RAD + 1, dtype=jnp.int32)
    pos_freq = jnp.arange(1, RAD + 1, dtype=jnp.int32)
    positions = jnp.arange(N, dtype=jnp.int32)
    cosine, sine_part = wave_tables(positions, all_freq)
    z_table = jnp.concatenate([cosine, sine_part], 1).astype(jnp.bfloat16)
    y_table = jnp.stack(
        [jnp.stack([cosine, sine_part], 1), jnp.stack([-sine_part, cosine], 1)], 1
    ).astype(jnp.bfloat16)
    x_cos, x_sin = wave_tables(x_positions, pos_freq)
    x_table = jnp.stack([jnp.stack([x_cos, -x_sin], 1), jnp.stack([-x_sin, -x_cos], 1)], 1).astype(
        jnp.bfloat16
    )
    return (z_table, y_table, x_table)


def pair_product(left_rows, right_rows):
    return lax.dot_general(
        left_rows, right_rows, (((0,), (0,)), ((), ())), preferred_element_type=jnp.float32
    )


def body(valence, conduction, val_energy, cond_energy, val_occupation, gvectors):
    pair_count = lax.axis_size("pair")
    gcol_count = lax.axis_size("gcol")
    planes = valence.shape[1]
    cond_bands = conduction.shape[0]
    extent = 2 * RAD + 1
    local_pairs = cond_bands * NV
    x_positions = lax.axis_index("grow") * planes + jnp.arange(planes, dtype=jnp.int32)
    z_table, y_table, x_table = build_tables(x_positions)
    flat_index = ((gvectors[0] - 1) * extent + gvectors[1] + RAD) * extent + gvectors[2] + RAD
    density = conduction[:, None] * valence[None]
    section_one = jnp.dot(
        density.reshape(-1, N), z_table, preferred_element_type=jnp.float32
    ).astype(jnp.bfloat16)
    section_one = section_one.reshape(local_pairs * planes, N, 2, extent)
    second = jnp.einsum(
        "ayik,yioj->aojk", section_one, y_table, preferred_element_type=jnp.float32
    ).astype(jnp.bfloat16)
    second = second.reshape(local_pairs, planes, 2, extent * extent)
    section_three = jnp.einsum(
        "pxoq,xosm->psmq", second, x_table, preferred_element_type=jnp.float32
    )
    section_three = section_three.reshape(local_pairs, 2, RAD * extent * extent)
    picked = jnp.take(section_three, flat_index, axis=2).reshape(local_pairs, 2 * KG)
    summed = lax.psum_scatter(
        picked.astype(jnp.bfloat16), "grow", scatter_dimension=1, tiled=True
    ).astype(jnp.float32)
    first_band = (lax.axis_index("pair") * gcol_count + lax.axis_index("gcol")) * cond_bands
    own_energy = lax.dynamic_slice_in_dim(cond_energy, first_band, cond_bands, 0)
    weight = val_occupation.astype(jnp.float32)[None, :] / (
        4.0 * (own_energy[:, None] - val_energy[None, :])
    )
    factor = (jnp.sqrt(weight) * (1.0 / N**1.5)).reshape(local_pairs, 1)
    weighted = (summed * factor).astype(jnp.bfloat16)
    prefactor = -1.0 / math.sqrt(pair_count * gcol_count * local_pairs)
    full_rows = lax.all_gather(weighted, "grow", axis=1, tiled=True)
    row_part = lax.all_to_all(full_rows, "pair", split_axis=1, concat_axis=0, tiled=True)
    partial_value = pair_product(row_part, lax.all_gather(weighted, "pair", axis=0, tiled=True))
    return lax.psum_scatter(
        (partial_value * prefactor).astype(jnp.bfloat16), "gcol", scatter_dimension=0, tiled=True
    ).astype(jnp.float32)


EXT = 2 * RAD + 1
QUARTER = N * N // 4
STEP = 8 * N
CLASSES = ((0, 4, 8, 12), (2, 6, 10), (1, 3, 5, 7, 9, 11))
WIDTHS = (128, 128, 256)
ROWS = (104, 80, 152)
STARTS = (0, 104, 184)
NR = 336


def half_plane_tables():
    total = 2 * sum(WIDTHS)
    left = np.zeros((2, N // 4, total), np.float32)
    right = np.zeros((2, N, total), np.float32)
    sign = np.zeros((1, WIDTHS[2]), np.float32)
    y = np.arange(N // 4)[:, None]
    z = np.arange(N)[:, None]
    k = np.arange(-RAD, RAD + 1)
    base = 0
    for freqs, width in zip(CLASSES, WIDTHS):
        jj = np.repeat(np.array(freqs), EXT)[None]
        kk = np.tile(k, len(freqs))[None]
        count = jj.shape[1]
        ay = 2 * np.pi * ((jj * y) % N) / N
        az = 2 * np.pi * ((kk * z) % N) / N
        for part in range(2):
            cols = slice(base + part * width, base + part * width + count)
            left[0, :, cols] = np.sin(ay) if part else np.cos(ay)
            left[1, :, cols] = np.cos(ay) if part else -np.sin(ay)
            right[0, :, cols] = np.cos(az)
            right[1, :, cols] = np.sin(az)
        base += 2 * width
    jj = np.repeat(np.array(CLASSES[2]), EXT)
    sign[0, : jj.size] = np.where(jj % 4 == 1, 1.0, -1.0)
    return left, right, sign


def plane_table(pairs):
    x = np.arange(N)[:, None]
    a = np.arange(1, RAD + 1)[None]
    ang = 2 * np.pi * ((a * x) % N) / N
    c, s = np.cos(ang), np.sin(ang)
    tab = np.stack([np.stack([c, -s, c, -s], -1), np.stack([-s, -c, s, c], -1)])
    return np.repeat(tab.reshape(2, N, RAD * 4), pairs, axis=2).astype(np.float32)


def chi_kernel(
    idx, occ, val_e, cond_e, v0, v1, v2, v3, c0, c1, c2, c3, left, right, sign, xtab,
    cols_out, rows_out,
    ee, eo, oo, tabs, acc_ee, acc_eo, acc_o, xmat, sec, got, part, inbox, blocks, cols, rows,
    sends, recvs, outs,
):
    band, step = pl.program_id(0), pl.program_id(1)
    bands, steps = part.shape[0], tabs.shape[0]
    nv, planes, _ = v0.shape
    height = nv * planes
    lanes = 128
    per_tile = lanes // (4 * nv)
    f32, bf16 = jnp.float32, jnp.bfloat16
    _, count, _, width = blocks.shape
    n = count - 1
    p, g, c = lax.axis_index("pair"), lax.axis_index("grow"), lax.axis_index("gcol")
    me = p * 2 + c
    turn = lambda at, k: lax.rem(at + k, count)
    block = lambda at: pl.ds(pl.multiple_of(at * width, 128), width)

    def copy_of(h, src, dst, sem, to):
        return pltpu.make_async_remote_copy(
            src_ref=src, dst_ref=dst, send_sem=sends.at[h, sem], recv_sem=recvs.at[h, sem],
            device_id=to, device_id_type=pl.DeviceIdType.MESH,
        )

    def first(h, k):
        return copy_of(
            h, part.at[h, :, block(turn(g, k))], inbox.at[h, k - 1], k - 1, (p, turn(g, k), c)
        )

    def along(h, k):
        return copy_of(h, blocks.at[h, g], blocks.at[h, g], n + k - 1, (p, turn(g, k), c))

    def flat(h, k):
        return copy_of(h, cols.at[me, h], cols.at[me, h], 2 * n + k - 1, (turn(p, k), g, c))

    def across(h, k):
        return copy_of(
            h, blocks.at[h, turn(p, k)], rows.at[me, h], 3 * n + k - 1, (turn(p, k), g, c)
        )

    def over(h, k, ref, base):
        slot = turn(p, count - k) * 2 + c
        return copy_of(h, ref.at[slot, h], ref.at[slot, h], base + k, (p, g, 1 - c))

    def stage_send(h):
        for k in range(1, count):
            first(h, k).start()

    def stage_sum(h):
        total = part[h, :, block(g)].astype(f32)
        for k in range(1, count):
            first(h, k).wait_recv()
            total += inbox[h, k - 1].astype(f32)
        mine = total.astype(bf16)
        blocks[h, g] = mine
        cols[me, h] = mine
        for k in range(1, count):
            along(h, k).start()
        for k in range(1, count):
            flat(h, k).start()
        over(h, 0, cols, 4 * n).start()

    def stage_across(h):
        for k in range(1, count):
            along(h, k).wait_recv()
        for k in range(1, count):
            across(h, k).start()
        rows[me, h] = blocks[h, p]
        over(h, 0, rows, 5 * n + 1).start()
        for k in range(1, count):
            flat(h, k).wait_recv()
            over(h, k, cols, 4 * n).start()

    def stage_rows(h):
        for k in range(1, count):
            across(h, k).wait_recv()
            over(h, k, rows, 5 * n + 1).start()

    @pl.when((band == 0) & (step == 0))
    def _():
        barrier = pltpu.get_barrier_semaphore()
        for k in range(1, count):
            pl.semaphore_signal(barrier, inc=1, device_id=(p, turn(g, k), c))
            pl.semaphore_signal(barrier, inc=1, device_id=(turn(p, k), g, c))
        pl.semaphore_signal(barrier, inc=1, device_id=(p, g, 1 - c))
        pl.semaphore_wait(barrier, 2 * count - 1)

    @pl.when(band == 0)
    def _():
        for y in range(STEP // N):
            yy = step * (STEP // N) + y
            l1 = left[0, pl.ds(yy, 1), :]
            l2 = left[1, pl.ds(yy, 1), :]
            tabs[step, y * N : (y + 1) * N, :] = (l1 * right[0] + l2 * right[1]).astype(bf16)

    @pl.when(step == 0)
    def _():
        acc_ee[...] = jnp.zeros_like(acc_ee)
        acc_eo[...] = jnp.zeros_like(acc_eo)
        acc_o[...] = jnp.zeros_like(acc_o)

    def products(v, carry):
        d0, d1, d2, d3 = [
            (a[pl.ds(2 * v, 2)].astype(f32) * b[band].astype(f32)[None]).reshape(2 * planes, STEP)
            for a, b in ((v0, c0), (v1, c1), (v2, c2), (v3, c3))
        ]
        e0, e1 = d0 + d2, d1 + d3
        at = pl.multiple_of(v * 2 * planes, 16)
        where = pl.ds(at, 2 * planes)
        ee[where, :] = (e0 + e1).astype(bf16)
        eo[where, :] = (e0 - e1).astype(bf16)
        oo[where, :] = (d0 - d2).astype(bf16)
        oo[pl.ds(pl.multiple_of(height + at, 16), 2 * planes), :] = (d1 - d3).astype(bf16)
        return carry

    lax.fori_loop(0, nv // 2, products, 0)
    acc_ee[...] += jnp.dot(ee[...], tabs[step, :, 0:256], preferred_element_type=f32)
    acc_eo[...] += jnp.dot(eo[...], tabs[step, :, 256:512], preferred_element_type=f32)

    def multiply(i, carry):
        at = pl.ds(pl.multiple_of(i * height, 16), height)
        acc_o[at, :] += jnp.dot(oo[at, :], tabs[step, :, 512:1024], preferred_element_type=f32)
        return carry

    lax.fori_loop(0, 2, multiply, 0)

    for h in range(1, bands):
        @pl.when((band == h) & (step == steps - 2))
        def _():
            stage_sum(h - 1)

        @pl.when((band == h) & (step == steps - 1))
        def _():
            stage_across(h - 1)

    @pl.when((band == 0) & (step == 0))
    def _():
        own = lax.broadcasted_iota(jnp.int32, (1, RAD * 4 * nv), 1) % nv

        weights = [xtab[h, pl.ds(pl.multiple_of(g * planes, 8), planes), :] for h in range(2)]

        def place(v, carry):
            for h in range(2):
                two = [jnp.where(own == 2 * v + u, weights[h], 0.0) for u in range(2)]
                at = pl.multiple_of(h * height + v * 2 * planes, 16)
                xmat[pl.ds(at, 2 * planes), :] = jnp.concatenate(two, 0).astype(bf16)
            return carry

        lax.fori_loop(0, nv // 2, place, 0)

    @pl.when(step == steps - 1)
    def _():
        lane = lax.broadcasted_iota(jnp.int32, (1, lanes), 1) % nv
        occupied = jnp.zeros((1, lanes), jnp.int32)
        energy = jnp.zeros((1, lanes), f32)
        for v in range(nv):
            occupied = jnp.where(lane == v, occ[v], occupied)
            energy = jnp.where(lane == v, val_e[v], energy)
        gap = cond_e[me * bands + band] - energy
        factor = jnp.sqrt(occupied.astype(f32) / (4.0 * gap)) * (1.0 / N**1.5)
        w = WIDTHS[2]
        top, low = acc_o[0:height, :], acc_o[height : 2 * height, :]
        odd_p = top[:, 0:w] - sign[...] * low[:, w:]
        odd_q = top[:, w:] + sign[...] * low[:, 0:w]
        groups = (
            (acc_ee[:, 0:128], acc_ee[:, 128:256]),
            (acc_eo[:, 0:128], acc_eo[:, 128:256]),
            (odd_p, odd_q),
        )
        for (p_part, q_part), size, start in zip(groups, ROWS, STARTS):
            p_rows = p_part.T[0:size].astype(bf16)
            q_rows = q_part.T[0:size].astype(bf16)
            summed = jnp.dot(p_rows, xmat[0:height, :], preferred_element_type=f32)
            summed += jnp.dot(q_rows, xmat[height : 2 * height, :], preferred_element_type=f32)
            for t in range(RAD // per_tile):
                piece = summed[:, t * lanes : (t + 1) * lanes] * factor
                for u in range(2 * per_tile):
                    a = t * per_tile + u // 2
                    at = ((u % 2) * RAD + a) * NR + start
                    turned = pltpu.roll(piece, lanes - 2 * nv * u, 1) if u else piece
                    sec[at : at + size, :] = turned

        def pick(i, carry):
            for u in range(16):
                got[pl.ds(i * 16 + u, 1), :] = sec[pl.ds(idx[i * 16 + u], 1), :]
            return carry

        lax.fori_loop(0, KG // 16, pick, 0)
        for i in range(KG // 384):
            turned = got[i * 384 : (i + 1) * 384, :].T.astype(bf16)
            part[band, :, i * 384 : (i + 1) * 384] = turned[0:nv]
            part[band, :, KG + i * 384 : KG + (i + 1) * 384] = turned[nv : 2 * nv]

    for h in range(bands):
        @pl.when((band == h) & (step == steps - 1))
        def _():
            stage_send(h)
            if h:
                stage_rows(h - 1)
            if h == bands - 1:
                stage_sum(h)
                stage_across(h)
                stage_rows(h)
                for q in range(bands):
                    for k in range(count):
                        over(q, k, cols, 4 * n).wait_recv()
                first_out = pltpu.make_async_copy(cols, cols_out, outs.at[0])
                first_out.start()
                for q in range(bands):
                    for k in range(count):
                        over(q, k, rows, 5 * n + 1).wait_recv()
                second_out = pltpu.make_async_copy(rows, rows_out, outs.at[1])
                second_out.start()
                for q in range(bands):
                    for k in range(1, count):
                        first(q, k).wait_send()
                        along(q, k).wait_send()
                        flat(q, k).wait_send()
                        across(q, k).wait_send()
                    for k in range(count):
                        over(q, k, cols, 4 * n).wait_send()
                        over(q, k, rows, 5 * n + 1).wait_send()
                first_out.wait()
                second_out.wait()


def row_index(gvectors):
    a, b, d = gvectors[0], gvectors[1], gvectors[2]
    flip = b < 0
    j = jnp.abs(b)
    k = jnp.where(flip, -d, d) + RAD
    row = jnp.where(
        j % 2 == 1,
        STARTS[2] + (j // 2) * EXT,
        jnp.where(j % 4 == 2, STARTS[1], STARTS[0]) + (j // 4) * EXT,
    )
    return (jnp.where(flip, RAD, 0) + a - 1) * NR + row + k


def fast_body(valence, conduction, val_energy, cond_energy, val_occupation, gvectors):
    nv, planes, _ = valence.shape
    bands = conduction.shape[0]
    count = lax.axis_size("pair")
    gcol_count = lax.axis_size("gcol")
    height = nv * planes
    steps = QUARTER // STEP
    width = 2 * KG // count
    slots = count * gcol_count
    bf16, f32 = jnp.bfloat16, jnp.float32
    left, right, sign = half_plane_tables()
    whole = lambda shape: pl.BlockSpec(shape, lambda b, i, idx: (0,) * len(shape))
    piece = lambda size, q: pl.BlockSpec(
        (size, planes, STEP), lambda b, i, idx, q=q: (0, 0, q * steps + i)
    )
    smem = pl.BlockSpec(memory_space=pltpu.SMEM)
    gathered = jax.ShapeDtypeStruct((slots, bands, nv, width), bf16)
    sems = 6 * (count - 1) + 2
    cols, rows = pl.pallas_call(
        chi_kernel,
        out_shape=(gathered, gathered),
        grid_spec=pltpu.PrefetchScalarGridSpec(
            num_scalar_prefetch=1,
            grid=(bands, steps),
            in_specs=[smem] * 3
            + [piece(nv, q) for q in range(4)]
            + [piece(bands, q) for q in range(4)]
            + [
                whole(left.shape),
                whole(right.shape),
                whole(sign.shape),
                whole((2, N, RAD * 4 * nv)),
            ],
            out_specs=(pl.BlockSpec(memory_space=pl.ANY), pl.BlockSpec(memory_space=pl.ANY)),
            scratch_shapes=[
                pltpu.VMEM((height, STEP), bf16),
                pltpu.VMEM((height, STEP), bf16),
                pltpu.VMEM((2 * height, STEP), bf16),
                pltpu.VMEM((steps, STEP, 2 * sum(WIDTHS)), bf16),
                pltpu.VMEM((height, 2 * WIDTHS[0]), f32),
                pltpu.VMEM((height, 2 * WIDTHS[1]), f32),
                pltpu.VMEM((2 * height, 2 * WIDTHS[2]), f32),
                pltpu.VMEM((2 * height, RAD * 4 * nv), bf16),
                pltpu.VMEM((2 * RAD * NR, 128), f32),
                pltpu.VMEM((KG, 128), f32),
                pltpu.VMEM((bands, nv, 2 * KG), bf16),
                pltpu.VMEM((bands, count - 1, nv, width), bf16),
                pltpu.VMEM((bands, count, nv, width), bf16),
                pltpu.VMEM((slots, bands, nv, width), bf16),
                pltpu.VMEM((slots, bands, nv, width), bf16),
                pltpu.SemaphoreType.DMA((bands, sems)),
                pltpu.SemaphoreType.DMA((bands, sems)),
                pltpu.SemaphoreType.DMA((2,)),
            ],
        ),
        compiler_params=pltpu.CompilerParams(
            vmem_limit_bytes=60 * 1024 * 1024, collective_id=0, has_side_effects=True
        ),
    )(
        row_index(gvectors), val_occupation, val_energy, cond_energy,
        *([valence] * 4), *([conduction] * 4), left, right, sign, plane_table(nv),
    )
    all_pairs = slots * bands * nv
    prefactor = -1.0 / math.sqrt(all_pairs)
    cols = cols.reshape(all_pairs, width)
    rows = rows.reshape(all_pairs, width)
    share = width // gcol_count
    rows = lax.dynamic_slice_in_dim(rows, lax.axis_index("gcol") * share, share, 1)
    return pair_product(rows, cols) * prefactor


def solution(mesh):
    sizes = dict(mesh.shape)
    fast = sizes["pair"] == sizes["grow"] and sizes["gcol"] == 2 and N // sizes["grow"] % 8 == 0
    return jax.shard_map(
        fast_body if fast else body,
        mesh=mesh,
        in_specs=(P(None, "grow", None), P(("pair", "gcol"), "grow", None), P(), P(), P(), P()),
        out_specs=P(("pair", "gcol"), "grow"),
        check_vma=False,
    )
```

```python
import functools
import math

import jax
import jax.numpy as jnp
import numpy as np
from jax import lax
from jax.experimental import pallas as pl
from jax.experimental.pallas import tpu as pltpu
from jax.sharding import PartitionSpec as P

N = 96
RAD = 12
KG = 3840
NV = 16


def wave_tables(positions, frequencies):
    phases = jnp.mod(positions[:, None] * frequencies[None, :], N).astype(jnp.float32) * (
        2.0 * math.pi / N
    )
    return (jnp.cos(phases), jnp.sin(phases))


def build_tables(x_positions):
    all_freq = jnp.arange(-RAD, RAD + 1, dtype=jnp.int32)
    pos_freq = jnp.arange(1, RAD + 1, dtype=jnp.int32)
    positions = jnp.arange(N, dtype=jnp.int32)
    cosine, sine_part = wave_tables(positions, all_freq)
    z_table = jnp.concatenate([cosine, sine_part], 1).astype(jnp.bfloat16)
    y_table = jnp.stack(
        [jnp.stack([cosine, sine_part], 1), jnp.stack([-sine_part, cosine], 1)], 1
    ).astype(jnp.bfloat16)
    x_cos, x_sin = wave_tables(x_positions, pos_freq)
    x_table = jnp.stack([jnp.stack([x_cos, -x_sin], 1), jnp.stack([-x_sin, -x_cos], 1)], 1).astype(
        jnp.bfloat16
    )
    return (z_table, y_table, x_table)


def pair_product(left_rows, right_rows):
    return lax.dot_general(
        left_rows, right_rows, (((0,), (0,)), ((), ())), preferred_element_type=jnp.float32
    )


def body(valence, conduction, val_energy, cond_energy, val_occupation, gvectors):
    pair_count = lax.axis_size("pair")
    gcol_count = lax.axis_size("gcol")
    planes = valence.shape[1]
    cond_bands = conduction.shape[0]
    extent = 2 * RAD + 1
    local_pairs = cond_bands * NV
    x_positions = lax.axis_index("grow") * planes + jnp.arange(planes, dtype=jnp.int32)
    z_table, y_table, x_table = build_tables(x_positions)
    flat_index = ((gvectors[0] - 1) * extent + gvectors[1] + RAD) * extent + gvectors[2] + RAD
    density = conduction[:, None] * valence[None]
    section_one = jnp.dot(
        density.reshape(-1, N), z_table, preferred_element_type=jnp.float32
    ).astype(jnp.bfloat16)
    section_one = section_one.reshape(local_pairs * planes, N, 2, extent)
    second = jnp.einsum(
        "ayik,yioj->aojk", section_one, y_table, preferred_element_type=jnp.float32
    ).astype(jnp.bfloat16)
    second = second.reshape(local_pairs, planes, 2, extent * extent)
    section_three = jnp.einsum(
        "pxoq,xosm->psmq", second, x_table, preferred_element_type=jnp.float32
    )
    section_three = section_three.reshape(local_pairs, 2, RAD * extent * extent)
    picked = jnp.take(section_three, flat_index, axis=2).reshape(local_pairs, 2 * KG)
    summed = lax.psum_scatter(
        picked.astype(jnp.bfloat16), "grow", scatter_dimension=1, tiled=True
    ).astype(jnp.float32)
    first_band = (lax.axis_index("pair") * gcol_count + lax.axis_index("gcol")) * cond_bands
    own_energy = lax.dynamic_slice_in_dim(cond_energy, first_band, cond_bands, 0)
    weight = val_occupation.astype(jnp.float32)[None, :] / (
        4.0 * (own_energy[:, None] - val_energy[None, :])
    )
    factor = (jnp.sqrt(weight) * (1.0 / N**1.5)).reshape(local_pairs, 1)
    weighted = (summed * factor).astype(jnp.bfloat16)
    prefactor = -1.0 / math.sqrt(pair_count * gcol_count * local_pairs)
    full_rows = lax.all_gather(weighted, "grow", axis=1, tiled=True)
    row_part = lax.all_to_all(full_rows, "pair", split_axis=1, concat_axis=0, tiled=True)
    partial_value = pair_product(row_part, lax.all_gather(weighted, "pair", axis=0, tiled=True))
    return lax.psum_scatter(
        (partial_value * prefactor).astype(jnp.bfloat16), "gcol", scatter_dimension=0, tiled=True
    ).astype(jnp.float32)


EXT = 2 * RAD + 1
QUARTER = N * N // 4
STEP = 8 * N
CLASSES = ((0, 4, 8, 12), (2, 6, 10), (1, 3, 5, 7, 9, 11))
WIDTHS = (128, 128, 256)
ROWS = (104, 80, 152)
STARTS = (0, 104, 184)
NR = 336


def half_plane_tables():
    total = 2 * sum(WIDTHS)
    left = np.zeros((2, N // 4, total), np.float32)
    right = np.zeros((2, N, total), np.float32)
    sign = np.zeros((1, WIDTHS[2]), np.float32)
    y = np.arange(N // 4)[:, None]
    z = np.arange(N)[:, None]
    k = np.arange(-RAD, RAD + 1)
    base = 0
    for freqs, width in zip(CLASSES, WIDTHS):
        jj = np.repeat(np.array(freqs), EXT)[None]
        kk = np.tile(k, len(freqs))[None]
        count = jj.shape[1]
        ay = 2 * np.pi * ((jj * y) % N) / N
        az = 2 * np.pi * ((kk * z) % N) / N
        for part in range(2):
            cols = slice(base + part * width, base + part * width + count)
            left[0, :, cols] = np.sin(ay) if part else np.cos(ay)
            left[1, :, cols] = np.cos(ay) if part else -np.sin(ay)
            right[0, :, cols] = np.cos(az)
            right[1, :, cols] = np.sin(az)
        base += 2 * width
    jj = np.repeat(np.array(CLASSES[2]), EXT)
    sign[0, : jj.size] = np.where(jj % 4 == 1, 1.0, -1.0)
    return left, right, sign


def plane_table(pairs):
    x = np.arange(N)[:, None]
    a = np.arange(1, RAD + 1)[None]
    ang = 2 * np.pi * ((a * x) % N) / N
    c, s = np.cos(ang), np.sin(ang)
    tab = np.stack([np.stack([c, -s, c, -s], -1), np.stack([-s, -c, s, c], -1)])
    return np.repeat(tab.reshape(2, N, RAD * 4), pairs, axis=2).astype(np.float32)


def row_index(a, b, d):
    flip = b < 0
    j = jnp.abs(b)
    k = jnp.where(flip, -d, d) + RAD
    row = jnp.where(
        (j & 1) == 1,
        STARTS[2] + (j >> 1) * EXT,
        jnp.where((j & 3) == 2, STARTS[1], STARTS[0]) + (j >> 2) * EXT,
    )
    return jnp.maximum((jnp.where(flip, RAD, 0) + a - 1) * NR + row + k, 0)


def chi_kernel(
    occ, val_e, cond_e, gvec, v0, v1, v2, v3, c0, c1, c2, c3, left, right, sign, xtab,
    cols_out, rows_out,
    ee, eo, oo, tabs, acc_ee, acc_eo, acc_o, xmat, sec, got, part, inbox, blocks, cols, rows,
    index, idx, sends, recvs, outs,
):
    band, step = pl.program_id(0), pl.program_id(1)
    bands, steps = part.shape[0], tabs.shape[0]
    nv, planes, _ = v0.shape
    height = nv * planes
    lanes = 128
    per_tile = lanes // (4 * nv)
    f32, bf16 = jnp.float32, jnp.bfloat16
    _, count, _, width = blocks.shape
    n = count - 1
    p, g, c = lax.axis_index("pair"), lax.axis_index("grow"), lax.axis_index("gcol")
    me = p * 2 + c
    turn = lambda at, k: lax.rem(at + k, count)
    block = lambda at: pl.ds(pl.multiple_of(at * width, 128), width)

    def copy_of(h, src, dst, sem, to):
        return pltpu.make_async_remote_copy(
            src_ref=src, dst_ref=dst, send_sem=sends.at[h, sem], recv_sem=recvs.at[h, sem],
            device_id=to, device_id_type=pl.DeviceIdType.MESH,
        )

    def first(h, k):
        return copy_of(
            h, part.at[h, :, block(turn(g, k))], inbox.at[h, k - 1], k - 1, (p, turn(g, k), c)
        )

    def along(h, k):
        return copy_of(h, blocks.at[h, g], blocks.at[h, g], n + k - 1, (p, turn(g, k), c))

    def flat(h, k):
        return copy_of(h, cols.at[me, h], cols.at[me, h], 2 * n + k - 1, (turn(p, k), g, c))

    def across(h, k):
        return copy_of(
            h, blocks.at[h, turn(p, k)], rows.at[me, h], 3 * n + k - 1, (turn(p, k), g, c)
        )

    def over(h, k, ref, base):
        slot = turn(p, count - k) * 2 + c
        return copy_of(h, ref.at[slot, h], ref.at[slot, h], base + k, (p, g, 1 - c))

    def pass_on(h, b):
        @pl.when(b != p)
        def _():
            copy_of(
                h, blocks.at[h, b], rows.at[me, h], 3 * n + turn(b, count - p) - 1, (b, g, c)
            ).start()

        @pl.when(b == p)
        def _():
            rows[me, h] = blocks[h, p]
            over(h, 0, rows, 5 * n + 1).start()

    def stage_sum(h):
        total = part[h, :, block(g)].astype(f32)
        for k in range(1, count):
            first(h, k).wait_recv()
            total += inbox[h, k - 1].astype(f32)
        mine = total.astype(bf16)
        blocks[h, g] = mine
        cols[me, h] = mine
        for k in range(1, count):
            along(h, k).start()
        for k in range(1, count):
            flat(h, k).start()
        over(h, 0, cols, 4 * n).start()
        pass_on(h, g)

    def stage_across(h):
        for k in range(1, count):
            flat(h, k).wait_recv()
            over(h, k, cols, 4 * n).start()
            along(h, k).wait_recv()
            pass_on(h, turn(g, count - k))

    def stage_rows(h):
        for k in range(1, count):
            across(h, k).wait_recv()
            over(h, k, rows, 5 * n + 1).start()

    @pl.when((band == 0) & (step == 0))
    def _():
        index[...] = row_index(gvec[0:1, :], gvec[1:2, :], gvec[2:3, :])
        pltpu.make_async_copy(index, idx, outs.at[0]).start()
        barrier = pltpu.get_barrier_semaphore()
        for k in range(1, count):
            pl.semaphore_signal(barrier, inc=1, device_id=(p, turn(g, k), c))
            pl.semaphore_signal(barrier, inc=1, device_id=(turn(p, k), g, c))
        pl.semaphore_signal(barrier, inc=1, device_id=(p, g, 1 - c))

    @pl.when(band == 0)
    def _():
        for y in range(STEP // N):
            yy = step * (STEP // N) + y
            l1 = left[0, pl.ds(yy, 1), :]
            l2 = left[1, pl.ds(yy, 1), :]
            tabs[step, y * N : (y + 1) * N, :] = (l1 * right[0] + l2 * right[1]).astype(bf16)

    @pl.when(step == 0)
    def _():
        acc_ee[...] = jnp.zeros_like(acc_ee)
        acc_eo[...] = jnp.zeros_like(acc_eo)
        acc_o[...] = jnp.zeros_like(acc_o)

    def products(v, carry):
        d0, d1, d2, d3 = [
            (a[pl.ds(2 * v, 2)].astype(f32) * b[band].astype(f32)[None]).reshape(2 * planes, STEP)
            for a, b in ((v0, c0), (v1, c1), (v2, c2), (v3, c3))
        ]
        e0, e1 = d0 + d2, d1 + d3
        at = pl.multiple_of(v * 2 * planes, 16)
        where = pl.ds(at, 2 * planes)
        ee[where, :] = (e0 + e1).astype(bf16)
        eo[where, :] = (e0 - e1).astype(bf16)
        oo[where, :] = (d0 - d2).astype(bf16)
        oo[pl.ds(pl.multiple_of(height + at, 16), 2 * planes), :] = (d1 - d3).astype(bf16)
        return carry

    lax.fori_loop(0, nv // 2, products, 0)
    acc_ee[...] += jnp.dot(ee[...], tabs[step, :, 0:256], preferred_element_type=f32)
    acc_eo[...] += jnp.dot(eo[...], tabs[step, :, 256:512], preferred_element_type=f32)

    def multiply(i, carry):
        at = pl.ds(pl.multiple_of(i * height, 16), height)
        acc_o[at, :] += jnp.dot(oo[at, :], tabs[step, :, 512:1024], preferred_element_type=f32)
        return carry

    lax.fori_loop(0, 2, multiply, 0)

    @pl.when((band == 0) & (step == steps - 1))
    def _():
        pltpu.make_async_copy(index, idx, outs.at[0]).wait()
        pl.semaphore_wait(pltpu.get_barrier_semaphore(), 2 * count - 1)

    for h in range(1, bands):
        @pl.when((band == h) & (step == steps - 2))
        def _():
            stage_sum(h - 1)

        @pl.when((band == h) & (step == steps - 1))
        def _():
            stage_across(h - 1)

    @pl.when((band == 0) & (step == 0))
    def _():
        own = lax.broadcasted_iota(jnp.int32, (1, RAD * 4 * nv), 1) % nv

        weights = [xtab[h, pl.ds(pl.multiple_of(g * planes, 8), planes), :] for h in range(2)]

        def place(v, carry):
            for h in range(2):
                two = [jnp.where(own == 2 * v + u, weights[h], 0.0) for u in range(2)]
                at = pl.multiple_of(h * height + v * 2 * planes, 16)
                xmat[pl.ds(at, 2 * planes), :] = jnp.concatenate(two, 0).astype(bf16)
            return carry

        lax.fori_loop(0, nv // 2, place, 0)

    @pl.when(step == steps - 1)
    def _():
        lane = lax.broadcasted_iota(jnp.int32, (1, lanes), 1) % nv
        occupied = jnp.zeros((1, lanes), jnp.int32)
        energy = jnp.zeros((1, lanes), f32)
        for v in range(nv):
            occupied = jnp.where(lane == v, occ[v], occupied)
            energy = jnp.where(lane == v, val_e[v], energy)
        gap = cond_e[me * bands + band] - energy
        factor = jnp.sqrt(occupied.astype(f32) / (4.0 * gap)) * (1.0 / N**1.5)
        w = WIDTHS[2]
        top, low = acc_o[0:height, :], acc_o[height : 2 * height, :]
        odd_p = top[:, 0:w] - sign[...] * low[:, w:]
        odd_q = top[:, w:] + sign[...] * low[:, 0:w]
        groups = (
            (acc_ee[:, 0:128], acc_ee[:, 128:256]),
            (acc_eo[:, 0:128], acc_eo[:, 128:256]),
            (odd_p, odd_q),
        )
        for (p_part, q_part), size, start in zip(groups, ROWS, STARTS):
            p_rows = p_part.T[0:size].astype(bf16)
            q_rows = q_part.T[0:size].astype(bf16)
            summed = jnp.dot(p_rows, xmat[0:height, :], preferred_element_type=f32)
            summed += jnp.dot(q_rows, xmat[height : 2 * height, :], preferred_element_type=f32)
            for t in range(RAD // per_tile):
                piece = summed[:, t * lanes : (t + 1) * lanes] * factor
                for u in range(2 * per_tile):
                    a = t * per_tile + u // 2
                    at = ((u % 2) * RAD + a) * NR + start
                    turned = pltpu.roll(piece, lanes - 2 * nv * u, 1) if u else piece
                    sec[at : at + size, :] = turned

        def pick(i, carry):
            for u in range(16):
                got[pl.ds(i * 16 + u, 1), :] = sec[pl.ds(idx[0, i * 16 + u], 1), :]
            return carry

        halves = KG // width
        for q in range(halves):
            lax.fori_loop(q * width // 16, (q + 1) * width // 16, pick, 0)
            for i in range(q * width // 384, (q + 1) * width // 384):
                turned = got[i * 384 : (i + 1) * 384, :].T.astype(bf16)
                part[band, :, i * 384 : (i + 1) * 384] = turned[0:nv]
                part[band, :, KG + i * 384 : KG + (i + 1) * 384] = turned[nv : 2 * nv]
            for k in range(1, count):
                @pl.when(lax.rem(turn(g, k), halves) == q)
                def _():
                    first(band, k).start()

    for h in range(bands):
        @pl.when((band == h) & (step == steps - 1))
        def _():
            if h:
                stage_rows(h - 1)
            if h == bands - 1:
                stage_sum(h)
                stage_across(h)
                stage_rows(h)
                for q in range(bands):
                    for k in range(count):
                        over(q, k, cols, 4 * n).wait_recv()
                first_out = pltpu.make_async_copy(cols, cols_out, outs.at[0])
                first_out.start()
                for q in range(bands):
                    for k in range(count):
                        over(q, k, rows, 5 * n + 1).wait_recv()
                second_out = pltpu.make_async_copy(rows, rows_out, outs.at[1])
                second_out.start()
                for q in range(bands):
                    for k in range(1, count):
                        first(q, k).wait_send()
                        along(q, k).wait_send()
                        flat(q, k).wait_send()
                        across(q, k).wait_send()
                    for k in range(count):
                        over(q, k, cols, 4 * n).wait_send()
                        over(q, k, rows, 5 * n + 1).wait_send()
                first_out.wait()
                second_out.wait()


def product_kernel(prefactor, rows, cols, out, turned):
    share, tile = out.shape
    c = lax.axis_index("gcol")
    low = share // 128 * 128
    shift = share - low

    @pl.when(pl.program_id(0) == 0)
    def _():
        span = turned.shape[0]
        turned[...] = rows[:, pl.ds(pl.multiple_of(c * low, 128), span)].T

    left = turned[pl.ds(pl.multiple_of(c * shift, 16), share), :]
    out[...] = jnp.dot(left, cols[...], preferred_element_type=jnp.float32) * prefactor


def product(rows, cols, share, prefactor):
    depth, width = rows.shape
    low = share // 128 * 128
    tile = 384
    return pl.pallas_call(
        functools.partial(product_kernel, prefactor),
        out_shape=jax.ShapeDtypeStruct((share, width), jnp.float32),
        grid=(width // tile,),
        in_specs=[
            pl.BlockSpec((depth, width), lambda i: (0, 0)),
            pl.BlockSpec((depth, tile), lambda i: (0, i)),
        ],
        out_specs=pl.BlockSpec((share, tile), lambda i: (0, i)),
        scratch_shapes=[pltpu.VMEM((width - low, depth), jnp.bfloat16)],
    )(rows, cols)


def fast_body(valence, conduction, val_energy, cond_energy, val_occupation, gvectors):
    nv, planes, _ = valence.shape
    bands = conduction.shape[0]
    count = lax.axis_size("pair")
    gcol_count = lax.axis_size("gcol")
    height = nv * planes
    steps = QUARTER // STEP
    width = 2 * KG // count
    slots = count * gcol_count
    bf16, f32 = jnp.bfloat16, jnp.float32
    left, right, sign = half_plane_tables()
    whole = lambda shape: pl.BlockSpec(shape, lambda b, i: (0,) * len(shape))
    piece = lambda size, q: pl.BlockSpec(
        (size, planes, STEP), lambda b, i, q=q: (0, 0, q * steps + i)
    )
    smem = pl.BlockSpec(memory_space=pltpu.SMEM)
    gathered = jax.ShapeDtypeStruct((slots, bands, nv, width), bf16)
    sems = 6 * (count - 1) + 2
    cols, rows = pl.pallas_call(
        chi_kernel,
        out_shape=(gathered, gathered),
        grid_spec=pltpu.PrefetchScalarGridSpec(
            num_scalar_prefetch=0,
            grid=(bands, steps),
            in_specs=[smem] * 3
            + [whole((3, KG))]
            + [piece(nv, q) for q in range(4)]
            + [piece(bands, q) for q in range(4)]
            + [
                whole(left.shape),
                whole(right.shape),
                whole(sign.shape),
                whole((2, N, RAD * 4 * nv)),
            ],
            out_specs=(pl.BlockSpec(memory_space=pl.ANY), pl.BlockSpec(memory_space=pl.ANY)),
            scratch_shapes=[
                pltpu.VMEM((height, STEP), bf16),
                pltpu.VMEM((height, STEP), bf16),
                pltpu.VMEM((2 * height, STEP), bf16),
                pltpu.VMEM((steps, STEP, 2 * sum(WIDTHS)), bf16),
                pltpu.VMEM((height, 2 * WIDTHS[0]), f32),
                pltpu.VMEM((height, 2 * WIDTHS[1]), f32),
                pltpu.VMEM((2 * height, 2 * WIDTHS[2]), f32),
                pltpu.VMEM((2 * height, RAD * 4 * nv), bf16),
                pltpu.VMEM((2 * RAD * NR, 128), f32),
                pltpu.VMEM((KG, 128), f32),
                pltpu.VMEM((bands, nv, 2 * KG), bf16),
                pltpu.VMEM((bands, count - 1, nv, width), bf16),
                pltpu.VMEM((bands, count, nv, width), bf16),
                pltpu.VMEM((slots, bands, nv, width), bf16),
                pltpu.VMEM((slots, bands, nv, width), bf16),
                pltpu.VMEM((1, KG), jnp.int32),
                pltpu.SMEM((1, KG), jnp.int32),
                pltpu.SemaphoreType.DMA((bands, sems)),
                pltpu.SemaphoreType.DMA((bands, sems)),
                pltpu.SemaphoreType.DMA((2,)),
            ],
        ),
        compiler_params=pltpu.CompilerParams(
            vmem_limit_bytes=60 * 1024 * 1024, collective_id=0, has_side_effects=True
        ),
    )(
        val_occupation, val_energy, cond_energy, gvectors,
        *([valence] * 4), *([conduction] * 4), left, right, sign, plane_table(nv),
    )
    all_pairs = slots * bands * nv
    prefactor = -1.0 / math.sqrt(all_pairs)
    cols = cols.reshape(all_pairs, width)
    rows = rows.reshape(all_pairs, width)
    share = width // gcol_count
    return product(rows, cols, share, prefactor)


def solution(mesh):
    sizes = dict(mesh.shape)
    fast = sizes["pair"] == sizes["grow"] and sizes["gcol"] == 2 and N // sizes["grow"] % 8 == 0
    return jax.shard_map(
        fast_body if fast else body,
        mesh=mesh,
        in_specs=(P(None, "grow", None), P(("pair", "gcol"), "grow", None), P(), P(), P(), P()),
        out_specs=P(("pair", "gcol"), "grow"),
        check_vma=False,
    )
```
